32 devices in a mesh: ep: 4 (over y, x), edp: 4 (over z), tp: 2 (over core).
Axes of the slice: x: 2, y: 2, z: 4, core: 2. Of those that a mesh axis runs over, the one named last changes fastest.
Arguments:
- tokens: bfloat16 [2048, 4096], P(('ep', 'edp'), 'tp'), may hold values from -6 to 6
- cotangent: bfloat16 [2048, 4096], P(('ep', 'edp'), 'tp'), may hold values from -6 to 6
- expert_ids: int32 [2048, 8], P(('ep', 'edp')), may hold values from 0 to 127, all different within a row; in each aligned block of 128 rows (0 to 127, 128 to 255, ...) at most 10 rows name the same one
- route_weights: float32 [2048, 8], P(('ep', 'edp')), may hold values from 0.1 to 1
- expert_weights: bfloat16 [3, 1536, 4096], P(None, ('ep', 'tp')), may hold values from -0.15625 to 0.15625
Outputs:
- mixed: bfloat16 [2048, 4096], P(('ep', 'edp'), 'tp')
- grad_tokens: bfloat16 [2048, 4096], P(('ep', 'edp'), 'tp')
- weight_grads: float32 [3, 1536, 4096], P(None, ('ep', 'tp'), 'edp')
The draws below stay inside these ranges and needn't reach their ends.
Inputs may be any that keep to these rules, and one draw needn't show every extreme that they name: `expert_ids`: each token names 8 different experts; within the tokens of one (ep, edp) index no expert is named by more than 10 tokens.
All inputs are finite; a program needn't handle non-finite values.
Results may differ from the reference program's by a relative error of at most 0.017.
Values may be sent and summed in bfloat16 or wider, within the bound.
A program may use at most 64 MiB of HBM per device.

```python
import math
import jax
import jax.numpy as jnp
import numpy as np
from jax import lax

D = 4096
FF = 1536
EXPERTS = 128
TOP = 8
TOK_DEV = 128
CAP = 10
EXP_WIN = 1
SLICE = 192
TOKENS = 2048
N_EP = 4
N_EDP = 4
N_TP = 2


def block_levels(key, extent, shards, least, high):
    factor_of = 1.0
    for axis_at, blocks in shards:
        heights = jax.random.uniform(jax.random.fold_in(jax.random.fold_in(key, 6), axis_at), (blocks,), jnp.float32, least / len(shards), high / len(shards))
        factor_of = factor_of * jnp.repeat(jnp.exp(heights), extent[axis_at] // blocks).reshape((-1,) + (1,) * (len(extent) - 1 - axis_at))
    return factor_of


def deal_out(rng, own, number, rows, count, top, limit, slope):
    sequence = jax.random.permutation(rng, count)
    heavy_load, common = load_shares(count, rows * top, limit, slope, True), load_shares(count, rows * top, limit, slope, False)
    places = jnp.arange(count)

    def named(sizes, turn):
        used = int((sizes > 0).sum())
        fixed = max(1, used // 4)
        passed = fixed + (places - fixed + turn * (used - fixed)) % max(1, count - fixed)
        return jnp.zeros((count,), jnp.int32).at[sequence[jnp.where(places < fixed, places, passed)]].set(jnp.asarray(sizes, jnp.int32))

    sizes = jnp.where(number % 4 == 0, named(heavy_load, number // 4), named(common, number - number // 4 - 1))
    mixed = jax.random.permutation(jax.random.fold_in(own, 3), count)
    donor, taker = mixed[0:count // 2 * 2:2], mixed[1:count // 2 * 2:2]
    margin = jnp.minimum(sizes[donor] - 1, limit - sizes[taker]) // 2
    margin = jnp.where((donor == sequence[0]) | (taker == sequence[0]) | (sizes[taker] == 0), 0, jnp.maximum(margin, 0))
    passed = jax.random.randint(jax.random.fold_in(own, 4), (count // 2,), 0, 1 << 20) % (margin + 1)
    sizes = sizes.at[donor].add(-passed).at[taker].add(passed)
    labels = jnp.searchsorted(jnp.cumsum(sizes), jnp.arange(rows * top), side="right").astype(jnp.int32)
    listing = labels.reshape(top, rows).T
    listing = listing[jax.random.permutation(jax.random.fold_in(own, 1), rows)]
    turn = jax.random.randint(jax.random.fold_in(own, 2), (rows, 1), 0, top)
    return jnp.take_along_axis(listing, (jnp.arange(top)[None, :] + turn) % top, axis=1)


def load_shares(count, total, bound, lean, full):
    loads = [(1 << 20) // math.isqrt(standing ** lean) + 1 for standing in range(1, count + 1)]
    largest = bound if full else min(bound, max(-(-total // count), total * loads[0] // sum(loads)))
    least = 1 if total - largest >= count - 1 else 0
    counts, surplus = [largest] + [least] * (count - 1), total - largest - least * (count - 1)
    while surplus > 0:
        movable = [i for i in range(1, count) if counts[i] < largest] or [i for i in range(1, count) if counts[i] < bound]
        pool, remaining = sum([loads[i] for i in movable]), surplus
        for i in movable:
            addition = min(bound - counts[i], max(1, remaining * loads[i] // pool), surplus)
            counts[i] = counts[i] + addition
            surplus = surplus - addition
    return np.array(counts)


def noise(rng, shape, width, most, cuts=(), held_as=jnp.bfloat16):
    loudness = block_levels(rng, shape, cuts, -0.22, 0.18) if cuts else 1.0
    result = jax.random.normal(rng, shape, jnp.float32) * width * loudness
    return jnp.minimum(jnp.maximum(result, -most), most).astype(held_as)


def setup_inputs(seed: int = 0) -> dict:
    splits = jax.random.split(jax.random.key(seed), 6)
    tokens = noise(splits[0], (TOKENS, D), 1.0, 6.0, ((0, 16), (1, 2)))
    cotangent = noise(splits[1], (TOKENS, D), 1.0, 6.0, ((0, 16), (1, 2)))
    expert_ids_keys = jax.random.split(jax.random.fold_in(splits[2], 1), TOKENS // TOK_DEV)
    expert_ids_turns = jax.random.permutation(jax.random.fold_in(splits[2], 3), TOKENS // TOK_DEV)
    expert_ids = jax.vmap(lambda own, number: deal_out(jax.random.fold_in(splits[2], 2), own, number, TOK_DEV, EXPERTS, TOP, CAP, 1))(expert_ids_keys, expert_ids_turns).reshape((TOKENS, TOP))
    route_weights = jnp.clip(jnp.exp(math.log(1.0) - 2.3025851 * jax.random.uniform(splits[3], (TOKENS, TOP), jnp.float32) ** block_levels(splits[3], (TOKENS, TOP), ((0, 16),), -0.2, 0.2)), 0.1, 1.0)
    expert_weights = noise(splits[4], (3, EXP_WIN * FF, D), FF ** -0.5, 0.15625, ((1, 8),))
    return {"tokens": tokens, "cotangent": cotangent, "expert_ids": expert_ids, "route_weights": route_weights, "expert_weights": expert_weights}


def settle(values):
    return lax.optimization_barrier(values.astype(jnp.bfloat16)).astype(jnp.float32)


def reference(tokens, cotangent, expert_ids, route_weights, expert_weights):
    groups = N_EP * N_EDP
    window = N_EP // 4
    per_group = TOK_DEV * TOP
    flat_ids = expert_ids.reshape(groups, per_group)
    matches = (flat_ids[:, :, None] == jnp.arange(window, dtype=jnp.int32)[None, None, :]).astype(jnp.int32)
    slot_index = jnp.sum(matches * (jnp.cumsum(matches, axis=1) - 1), axis=2).astype(jnp.int32)
    owner = jnp.where(jnp.sum(matches, axis=2) > 0, flat_ids, window).astype(jnp.int32)
    token_index = (jnp.arange(groups, dtype=jnp.int32)[:, None] * TOK_DEV
                   + jnp.arange(per_group, dtype=jnp.int32)[None, :] // TOP).astype(jnp.int32)
    group_index = jnp.broadcast_to(jnp.arange(groups, dtype=jnp.int32)[:, None], flat_ids.shape).astype(jnp.int32)
    slot_token = jnp.zeros((window, groups, CAP), jnp.int32).at[owner, group_index, slot_index].set(token_index, mode="drop")
    slot_weight = jnp.zeros((window, groups, CAP), jnp.float32).at[owner, group_index, slot_index].set(
        route_weights.reshape(groups, per_group), mode="drop")
    slot_live = jnp.zeros((window, groups, CAP), jnp.float32).at[owner, group_index, slot_index].set(
        jnp.ones((groups, per_group), jnp.float32), mode="drop")
    expert_blocks = jnp.moveaxis(expert_weights.reshape(3, window, 4, N_TP, SLICE, D), 1, 0)
    row_count = groups * CAP

    def one_expert(operands):
        slot_toks, slot_wts, slot_flags, blocks = operands
        flat_tok = slot_toks.reshape(-1)
        live_col = slot_flags.reshape(-1, 1)
        rows = tokens[flat_tok] * live_col.astype(jnp.bfloat16)
        scaled = (cotangent[flat_tok].astype(jnp.float32) * (slot_wts.reshape(-1, 1) * live_col)).astype(jnp.bfloat16)
        rows_wide = rows.astype(jnp.float32).reshape(N_EP, N_EDP, CAP, D)
        scaled_wide = scaled.astype(jnp.float32).reshape(N_EP, N_EDP, CAP, D)

        def per_replica(left, right_wide):
            left_wide = left.astype(jnp.float32).reshape(N_EP, N_EDP, CAP, SLICE)
            partial_sums = jnp.einsum("pics,picd->isd", left_wide, right_wide, precision=lax.Precision.HIGHEST)
            return jnp.sum(settle(partial_sums), axis=0)

        def one_slice(carry, slab):
            out_acc, back_acc = carry
            gate_w, up_w, down_w = slab[0], slab[1], slab[2]
            gate_val = jnp.dot(rows, gate_w.T, preferred_element_type=jnp.float32)
            up_val = jnp.dot(rows, up_w.T, preferred_element_type=jnp.float32)
            sigmoid_gate = jax.nn.sigmoid(gate_val)
            active = gate_val * sigmoid_gate
            hidden = (active * up_val).astype(jnp.bfloat16)
            out_part = jnp.dot(hidden, down_w, preferred_element_type=jnp.float32)
            d_hidden = jnp.dot(scaled, down_w.T, preferred_element_type=jnp.float32)
            d_gate = (d_hidden * up_val * sigmoid_gate * (1.0 + gate_val * (1.0 - sigmoid_gate))).astype(jnp.bfloat16)
            d_up = (d_hidden * active).astype(jnp.bfloat16)
            back_part = (jnp.dot(d_gate, gate_w, preferred_element_type=jnp.float32)
                         + jnp.dot(d_up, up_w, preferred_element_type=jnp.float32))
            grad_slab = jnp.stack([per_replica(d_gate, rows_wide), per_replica(d_up, rows_wide),
                                   per_replica(hidden, scaled_wide)])
            return (out_acc + settle(out_part), back_acc + settle(back_part)), grad_slab

        out_total = jnp.zeros((row_count, D), jnp.float32)
        back_total = jnp.zeros((row_count, D), jnp.float32)
        grad_list = []
        for half_index in range(4):
            start = (jnp.zeros((row_count, D), jnp.float32), jnp.zeros((row_count, D), jnp.float32))
            slabs = jnp.moveaxis(blocks[:, half_index], 1, 0)
            (out_half, back_half), grad_half = lax.scan(one_slice, start, slabs)
            out_total = out_total + settle(out_half)
            back_total = back_total + settle(back_half)
            grad_list.append(grad_half)
        return out_total, back_total, jnp.stack(grad_list)

    outs, backs, grads = lax.map(one_expert, (slot_token, slot_weight, slot_live, expert_blocks))
    weight_grads = jnp.moveaxis(grads, 3, 0).reshape(3, window * FF, D)
    flat_tok = slot_token.reshape(-1)
    mixed = jnp.zeros((groups * TOK_DEV, D), jnp.float32).at[flat_tok].add(
        (slot_weight * slot_live).reshape(-1, 1) * outs.reshape(-1, D)).astype(jnp.bfloat16)
    grad_tokens = jnp.zeros((groups * TOK_DEV, D), jnp.float32).at[flat_tok].add(
        slot_live.reshape(-1, 1) * backs.reshape(-1, D)).astype(jnp.bfloat16)
    return mixed, grad_tokens, weight_grads
```

```python
import functools

import jax
import jax.numpy as jnp
import numpy as np
from jax import lax
from jax.experimental import pallas as pl
from jax.experimental.pallas import tpu as pltpu
from jax.sharding import PartitionSpec as P

CAP = 10
PARTS = 4
MESH = pl.DeviceIdType.MESH
F32 = jnp.float32
BF16 = jnp.bfloat16


def round_up(value, unit):
    return -(-value // unit) * unit


class Sizes:
    def __init__(self, ep, edp, tp, tok_rows, feats, hid):
        self.ep, self.edp, self.tp = ep, edp, tp
        self.window = ep // PARTS
        self.tok_rows, self.feats, self.hid = tok_rows, feats, hid
        self.block = feats * tp // edp
        self.nblk = feats // self.block
        self.nch = max(1, min(4, self.block // 128))
        self.cw = self.block // self.nch
        self.xr = round_up(2 * CAP * self.nch, 16)
        self.rows = round_up(ep * CAP, 16)


def permutation(z):
    table = np.zeros((z.nch, 2, z.rows, z.ep, z.xr), np.float32)
    for q in range(z.nch):
        for a in range(2):
            for i in range(z.ep):
                for c in range(CAP):
                    table[q, a, i * CAP + c, i, (2 * q + a) * CAP + c] = 1.0
    flat = table.reshape(z.nch, 2 * z.rows, z.ep * z.xr)
    return flat.reshape(-1, z.ep * z.xr), np.swapaxes(flat, 1, 2).copy()


def slot_parts(index, nch):
    chunk = jnp.zeros_like(index)
    for k in range(1, nch):
        chunk += (index >= 2 * CAP * k).astype(jnp.int32)
    rest = index - 2 * CAP * chunk
    array = (rest >= CAP).astype(jnp.int32)
    return chunk, array, rest - CAP * array


def kernel(
    z, tok, cot, ids, rw, perm, perm_t, weights,
    mixed, grad_tok, wgrad,
    wb, x, xin, rb, rows, pout, pin, hb, lb, ob, y, yin, right,
    w_loc, w_send, w_recv, x_send, x_recv, r_send, r_recv, p_send, p_recv,
    l_send, l_recv, y_send, y_recv, q_send, q_recv,
):
    i, e, s = lax.axis_index("ep"), lax.axis_index("edp"), lax.axis_index("tp")
    barrier = pltpu.get_barrier_semaphore()
    group = z.ep * z.edp

    def greet(step, carry):
        di = step // z.edp
        de = step - di * z.edp
        pl.semaphore_signal(
            barrier, inc=1,
            device_id=(lax.rem(i + di, z.ep), lax.rem(e + de, z.edp), s),
            device_id_type=MESH,
        )
        return carry

    for d in range(1, z.tp):
        pl.semaphore_signal(
            barrier, inc=1, device_id=(i, e, lax.rem(s + d, z.tp)), device_id_type=MESH
        )
    lax.fori_loop(1, group, greet, 0)

    own_w = pltpu.make_async_copy(
        weights.at[:, :, pl.ds(pl.multiple_of(s * z.feats, 128), z.feats)], wb.at[s], w_loc
    )
    own_w.start()

    ids_t = jnp.transpose(ids[...].astype(F32))
    rw_t = jnp.transpose(rw[...])
    top = ids_t.shape[0]
    row = lax.broadcasted_iota(jnp.int32, (z.xr, z.tok_rows), 0)
    chunk, array, slot = slot_parts(row, z.nch)
    in_use = row < 2 * CAP * z.nch
    before = (
        lax.broadcasted_iota(jnp.int32, (z.tok_rows, z.tok_rows), 0)
        < lax.broadcasted_iota(jnp.int32, (z.tok_rows, z.tok_rows), 1)
    ).astype(F32).astype(BF16)
    picks, scales = [], []
    for w in range(z.window):
        hit = (ids_t == float(w)).astype(F32)
        match = jnp.sum(hit, axis=0, keepdims=True)
        weight = jnp.sum(hit * rw_t, axis=0, keepdims=True)
        match_all = jnp.broadcast_to(match, (z.xr, z.tok_rows))
        rank = jnp.dot(match_all.astype(BF16), before, preferred_element_type=F32)
        pick = jnp.where(in_use & (rank == slot.astype(F32)), match_all, 0.0)
        slot_weight = jnp.sum(pick * weight, axis=1, keepdims=True)
        scale = jnp.where(array[:, :1] == 1, slot_weight, 1.0)
        picks.append(pick)
        scales.append(jnp.where(array[:, :1] == 0, slot_weight, 1.0))
        for b in range(z.nblk):
            total = jnp.zeros((z.xr, z.cw), F32)
            for q in range(z.nch):
                cols = pl.ds(b * z.block + q * z.cw, z.cw)
                for a, source in ((0, tok), (1, cot)):
                    chosen = jnp.where((chunk == q) & (array == a), pick, 0.0).astype(BF16)
                    total += jnp.dot(chosen, source[:, cols], preferred_element_type=F32)
            x[w, b] = (total * scale).astype(BF16)

    pl.semaphore_wait(barrier, group - 1 + z.tp - 1)

    w_copies = []
    for d in range(1, z.tp):
        to = lax.rem(s + d, z.tp)
        w_copies.append(pltpu.make_async_remote_copy(
            src_ref=weights.at[:, :, pl.ds(pl.multiple_of(to * z.feats, 128), z.feats)],
            dst_ref=wb.at[s], send_sem=w_send.at[d], recv_sem=w_recv.at[s],
            device_id=(i, e, to), device_id_type=MESH,
        ))
    x_copies = []
    for d in range(1, z.ep):
        to = lax.rem(i + d, z.ep)
        x_copies.append(pltpu.make_async_remote_copy(
            src_ref=x.at[to // PARTS], dst_ref=xin.at[i],
            send_sem=x_send.at[d], recv_sem=x_recv.at[i],
            device_id=(to, e, s), device_id_type=MESH,
        ))
    for copy in x_copies + w_copies:
        copy.start()

    def right_copy(b, d):
        to = lax.rem(i + d, z.ep)
        return pltpu.make_async_remote_copy(
            src_ref=x.at[to // PARTS, b], dst_ref=rb.at[e, i],
            send_sem=r_send.at[b * z.ep + d], recv_sem=r_recv.at[0],
            device_id=(to, s * z.nblk + b, s), device_id_type=MESH,
        )

    for b in range(z.nblk):
        @pl.when(s * z.nblk + b != e)
        def _():
            for d in range(z.ep):
                right_copy(b, d).start()

    xin[i] = x[i // PARTS]
    for d in range(1, z.ep):
        source = lax.rem(i + d, z.ep)
        pltpu.make_async_copy(xin.at[source], xin.at[source], x_recv.at[source]).wait()

    arrange = perm[...]

    def unpack(packed):
        return jnp.dot(arrange, packed, preferred_element_type=F32).astype(BF16)

    for b in range(z.nblk):
        flat = unpack(xin[:, b].reshape(z.ep * z.xr, z.cw))
        for q in range(z.nch):
            cols = pl.ds(b * z.block + q * z.cw, z.cw)
            rows[:, cols] = flat[q * 2 * z.rows:(q + 1) * 2 * z.rows]

    own_w.wait()
    for d in range(1, z.tp):
        source = lax.rem(s + d, z.tp)
        pltpu.make_async_copy(wb.at[source], wb.at[source], w_recv.at[source]).wait()

    last = (((1,), (1,)), ((), ()))
    for t in range(z.tp):
        for m in range(3):
            part = rows[:z.rows] if m < 2 else rows[z.rows:]
            pout[t, m] = lax.dot_general(part, wb[t, m], last, preferred_element_type=F32)
    p_copies = []
    for d in range(1, z.tp):
        to = lax.rem(s + d, z.tp)
        copy = pltpu.make_async_remote_copy(
            src_ref=pout, dst_ref=pin.at[s], send_sem=p_send.at[d], recv_sem=p_recv.at[s],
            device_id=(i, e, to), device_id_type=MESH,
        )
        copy.start()
        p_copies.append(copy)
    for d in range(1, z.tp):
        source = lax.rem(s + d, z.tp)
        pltpu.make_async_copy(pin.at[source], pin.at[source], p_recv.at[source]).wait()

    for t in range(z.tp):
        sums = []
        for m in range(3):
            value = pout[t, m]
            for d in range(1, z.tp):
                value += pin[lax.rem(s + d, z.tp), t, m]
            sums.append(value)
        gate, up, d_hidden = sums
        sig = jax.nn.sigmoid(gate)
        active = gate * sig
        hb[t, 0] = (d_hidden * up * sig * (1.0 + gate * (1.0 - sig))).astype(BF16)
        hb[t, 1] = (d_hidden * active).astype(BF16)
        hb[t, 2] = (active * up).astype(BF16)

    l_copies = []
    for d in range(1, z.edp):
        copy = pltpu.make_async_remote_copy(
            src_ref=hb.at[s], dst_ref=lb.at[e], send_sem=l_send.at[d], recv_sem=l_recv.at[e],
            device_id=(i, lax.rem(e + d, z.edp), s), device_id_type=MESH,
        )
        copy.start()
        l_copies.append(copy)
    lb[e] = hb[s]

    out = jnp.zeros((z.rows, z.feats), F32)
    back = jnp.zeros((z.rows, z.feats), F32)
    for t in range(z.tp):
        out += jnp.dot(hb[t, 2], wb[t, 2], preferred_element_type=F32)
        back += jnp.dot(hb[t, 0], wb[t, 0], preferred_element_type=F32)
        back += jnp.dot(hb[t, 1], wb[t, 1], preferred_element_type=F32)
    ob[:z.rows] = out.astype(BF16)
    ob[z.rows:] = back.astype(BF16)
    for b in range(z.nblk):
        total = jnp.zeros((z.ep * z.xr, z.cw), F32)
        for q in range(z.nch):
            cols = pl.ds(b * z.block + q * z.cw, z.cw)
            total += jnp.dot(perm_t[q], ob[:, cols], preferred_element_type=F32)
        y[:, b] = total.astype(BF16).reshape(z.ep, z.xr, z.cw)
    y_copies = []
    for d in range(1, z.ep):
        to = lax.rem(i + d, z.ep)
        copy = pltpu.make_async_remote_copy(
            src_ref=y.at[to], dst_ref=yin.at[i], send_sem=y_send.at[d], recv_sem=y_recv.at[i],
            device_id=(to, e, s), device_id_type=MESH,
        )
        copy.start()
        y_copies.append(copy)
    yin[i] = y[i]

    owner = e // z.nblk
    mine = e - owner * z.nblk

    def relay(d):
        return pltpu.make_async_remote_copy(
            src_ref=rb, dst_ref=rb, send_sem=q_send.at[d], recv_sem=q_recv.at[0],
            device_id=(i, e, lax.rem(s + d, z.tp)), device_id_type=MESH,
        )

    @pl.when(s == owner)
    def _():
        for source in range(z.ep):
            rb[e, source] = xin[source, mine]
        others = rb.at[pl.ds(0, z.edp - 1)]
        pltpu.make_async_copy(others, others, r_recv.at[0]).wait()
        for d in range(1, z.tp):
            relay(d).start()

    @pl.when(s != owner)
    def _():
        pltpu.make_async_copy(rb, rb, q_recv.at[0]).wait()

    for r in range(z.edp):
        flat = unpack(rb[r].reshape(z.ep * z.xr, z.cw))
        for q in range(z.nch):
            for a in range(2):
                at = (2 * q + a) * z.rows
                right[a, pl.ds(r * z.rows, z.rows), pl.ds(q * z.cw, z.cw)] = flat[at:at + z.rows]

    for d in range(1, z.ep):
        source = lax.rem(i + d, z.ep)
        pltpu.make_async_copy(yin.at[source], yin.at[source], y_recv.at[source]).wait()

    lane = lax.broadcasted_iota(jnp.int32, (z.tok_rows, z.xr), 1)
    lane_chunk, lane_array, _ = slot_parts(lane, z.nch)
    homes = [jnp.transpose(pick) for pick in picks]
    for b in range(z.nblk):
        sums = []
        for w in range(z.window):
            total = yin[w * PARTS, b].astype(F32)
            for h in range(1, PARTS):
                total += yin[w * PARTS + h, b].astype(F32)
            sums.append((total * scales[w]).astype(BF16))
        for q in range(z.nch):
            cols = pl.ds(b * z.block + q * z.cw, z.cw)
            for a, target in ((0, mixed), (1, grad_tok)):
                value = jnp.zeros((z.tok_rows, z.cw), F32)
                for w in range(z.window):
                    chosen = jnp.where((lane_chunk == q) & (lane_array == a), homes[w], 0.0).astype(BF16)
                    value += jnp.dot(chosen, sums[w], preferred_element_type=F32)
                target[:, cols] = value.astype(BF16)

    for d in range(1, z.edp):
        source = lax.rem(e + d, z.edp)
        pltpu.make_async_copy(lb.at[source], lb.at[source], l_recv.at[source]).wait()
    first = (((0,), (0,)), ((), ()))
    for m in range(3):
        left = lb[:, m].reshape(z.edp * z.rows, z.hid)
        wgrad[m] = lax.dot_general(left, right[1 if m == 2 else 0], first, preferred_element_type=F32)

    for copy in x_copies + w_copies + p_copies + l_copies + y_copies:
        copy.wait_send()
    for b in range(z.nblk):
        @pl.when(s * z.nblk + b != e)
        def _():
            for d in range(z.ep):
                right_copy(b, d).wait_send()

    @pl.when(s == owner)
    def _():
        for d in range(1, z.tp):
            relay(d).wait_send()


def shards(tokens, cotangent, expert_ids, route_weights, expert_weights):
    z = Sizes(
        lax.axis_size("ep"), lax.axis_size("edp"), lax.axis_size("tp"),
        tokens.shape[0], tokens.shape[1], expert_weights.shape[1],
    )
    perm, perm_t = permutation(z)
    vmem = pl.BlockSpec(memory_space=pltpu.VMEM)
    dma = pltpu.SemaphoreType.DMA
    return pl.pallas_call(
        functools.partial(kernel, z),
        out_shape=(
            jax.ShapeDtypeStruct(tokens.shape, BF16),
            jax.ShapeDtypeStruct(tokens.shape, BF16),
            jax.ShapeDtypeStruct((3, z.hid, z.block), F32),
        ),
        in_specs=[vmem] * 6 + [pl.BlockSpec(memory_space=pltpu.HBM)],
        out_specs=(vmem,) * 3,
        scratch_shapes=[
            pltpu.VMEM((z.tp, 3, z.hid, z.feats), BF16),
            pltpu.VMEM((z.window, z.nblk, z.xr, z.cw), BF16),
            pltpu.VMEM((z.ep, z.nblk, z.xr, z.cw), BF16),
            pltpu.VMEM((z.edp, z.ep, z.xr, z.cw), BF16),
            pltpu.VMEM((2 * z.rows, z.feats), BF16),
            pltpu.VMEM((z.tp, 3, z.rows, z.hid), F32),
            pltpu.VMEM((z.tp, z.tp, 3, z.rows, z.hid), F32),
            pltpu.VMEM((z.tp, 3, z.rows, z.hid), BF16),
            pltpu.VMEM((z.edp, 3, z.rows, z.hid), BF16),
            pltpu.VMEM((2 * z.rows, z.feats), BF16),
            pltpu.VMEM((z.ep, z.nblk, z.xr, z.cw), BF16),
            pltpu.VMEM((z.ep, z.nblk, z.xr, z.cw), BF16),
            pltpu.VMEM((2, z.edp * z.rows, z.block), BF16),
            dma, dma((z.tp,)), dma((z.tp,)), dma((z.ep,)), dma((z.ep,)),
            dma((z.nblk * z.ep,)), dma((1,)), dma((z.tp,)), dma((z.tp,)),
            dma((z.edp,)), dma((z.edp,)), dma((z.ep,)), dma((z.ep,)),
            dma((z.tp,)), dma((1,)),
        ],
        compiler_params=pltpu.CompilerParams(
            collective_id=0, has_side_effects=True, vmem_limit_bytes=60 * 1024 * 1024
        ),
        name="expert_block",
    )(
        tokens, cotangent, expert_ids, route_weights,
        jnp.asarray(perm, BF16), jnp.asarray(perm_t, BF16), expert_weights,
    )


def solution(mesh):
    placed = (
        P(("ep", "edp"), "tp"),
        P(("ep", "edp"), "tp"),
        P(("ep", "edp"), None),
        P(("ep", "edp"), None),
        P(None, ("ep", "tp"), None),
    )
    return jax.shard_map(
        shards,
        mesh=mesh,
        in_specs=placed,
        out_specs=(P(("ep", "edp"), "tp"), P(("ep", "edp"), "tp"), P(None, ("ep", "tp"), "edp")),
        check_vma=False,
    )
```

```python
import functools

import jax
import jax.numpy as jnp
import numpy as np
from jax import lax
from jax.experimental import pallas as pl
from jax.experimental.pallas import tpu as pltpu
from jax.sharding import PartitionSpec as P

CAP = 10
PARTS = 4
VMEM_LIMIT = 61 * 1024 * 1024
MESH = pl.DeviceIdType.MESH
F32 = jnp.float32
BF16 = jnp.bfloat16


def round_up(value, unit):
    return -(-value // unit) * unit


class Sizes:
    def __init__(self, ep, edp, tp, tok_rows, feats, hid):
        self.ep, self.edp, self.tp = ep, edp, tp
        self.window = ep // PARTS
        self.tok_rows, self.feats, self.hid = tok_rows, feats, hid
        self.block = feats * tp // edp
        self.nblk = feats // self.block
        self.nch = max(1, min(4, self.block // 128))
        self.cw = self.block // self.nch
        self.xr = round_up(2 * CAP * self.nch, 16)
        self.rows = round_up(ep * CAP, 16)
        self.lanes = round_up(3 * ep * CAP, 128)


def permutations(z):
    table = np.zeros((z.nch, 2, z.rows, z.ep, z.xr), np.float32)
    factor = np.zeros((z.nch, z.lanes, z.ep, z.xr), np.float32)
    place = np.zeros((3, z.rows, z.lanes), np.float32)
    for i in range(z.ep):
        for c in range(CAP):
            for q in range(z.nch):
                for a in range(2):
                    table[q, a, i * CAP + c, i, (2 * q + a) * CAP + c] = 1.0
                for m in range(3):
                    factor[q, (m * z.ep + i) * CAP + c, i, (2 * q + m // 2) * CAP + c] = 1.0
            for m in range(3):
                place[m, i * CAP + c, (m * z.ep + i) * CAP + c] = 1.0
    flat = table.reshape(z.nch, 2 * z.rows, z.ep * z.xr)
    return (
        flat.reshape(-1, z.ep * z.xr), np.swapaxes(flat, 1, 2).copy(),
        factor.reshape(-1, z.ep * z.xr), place,
    )


def slot_parts(index, nch):
    chunk = jnp.zeros_like(index)
    for k in range(1, nch):
        chunk += (index >= 2 * CAP * k).astype(jnp.int32)
    rest = index - 2 * CAP * chunk
    array = (rest >= CAP).astype(jnp.int32)
    return chunk, array, rest - CAP * array


def kernel(
    z, tok_in, cot_in, ids_in, rw_in, perm_in, perm_t_in, factor_in, place_in, weights,
    left, right, summed, homes,
    tok, cot, ids, rw, perm, perm_t, factor, place,
    wb, x, xin, rb, rows, pout, pin, hb, lout, lb, ob, y, yin,
    in_sem, w_loc, w_send, w_recv, x_send, x_recv, r_send, r_recv, p_send, p_recv,
    l_send, l_recv, y_send, y_recv, q_send, q_recv,
):
    i, e, s = lax.axis_index("ep"), lax.axis_index("edp"), lax.axis_index("tp")
    barrier = pltpu.get_barrier_semaphore()
    group = z.ep * z.edp

    loads = [
        pltpu.make_async_copy(source, target, in_sem.at[k])
        for k, (source, target) in enumerate((
            (ids_in, ids), (rw_in, rw), (tok_in, tok), (cot_in, cot),
            (perm_in, perm), (perm_t_in, perm_t), (factor_in, factor), (place_in, place),
        ))
    ]
    for copy in loads[:4]:
        copy.start()

    def greet(step, carry):
        di = step // z.edp
        de = step - di * z.edp
        pl.semaphore_signal(
            barrier, inc=1,
            device_id=(lax.rem(i + di, z.ep), lax.rem(e + de, z.edp), s),
            device_id_type=MESH,
        )
        return carry

    for d in range(1, z.tp):
        pl.semaphore_signal(
            barrier, inc=1, device_id=(i, e, lax.rem(s + d, z.tp)), device_id_type=MESH
        )
    lax.fori_loop(1, group, greet, 0)

    own_w = pltpu.make_async_copy(
        weights.at[:, :, pl.ds(pl.multiple_of(s * z.feats, 128), z.feats)], wb.at[s], w_loc
    )
    own_w.start()
    for copy in loads[4:]:
        copy.start()

    row = lax.broadcasted_iota(jnp.int32, (z.xr, z.tok_rows), 0)
    chunk, array, slot = slot_parts(row, z.nch)
    in_use = row < 2 * CAP * z.nch
    before = (
        lax.broadcasted_iota(jnp.int32, (z.tok_rows, z.tok_rows), 0)
        < lax.broadcasted_iota(jnp.int32, (z.tok_rows, z.tok_rows), 1)
    ).astype(F32).astype(BF16)
    lane = lax.broadcasted_iota(jnp.int32, (z.tok_rows, z.xr), 1)
    lane_chunk, lane_array, _ = slot_parts(lane, z.nch)
    loads[0].wait()
    loads[1].wait()
    ids_t = ids[...]
    rw_t = rw[...]
    chosen, scales, picks = [], [], []
    for w in range(z.window):
        hit = (ids_t == w).astype(F32)
        match = jnp.sum(hit, axis=0, keepdims=True)
        weight = jnp.sum(hit * rw_t, axis=0, keepdims=True)
        match_all = jnp.broadcast_to(match, (z.xr, z.tok_rows))
        rank = jnp.dot(match_all.astype(BF16), before, preferred_element_type=F32)
        pick = jnp.where(in_use & (rank == slot.astype(F32)), match_all, 0.0)
        slot_weight = jnp.sum(pick * weight, axis=1, keepdims=True)
        picks.append(pick)
        scales.append((
            jnp.where(array[:, :1] == 1, slot_weight, 1.0), jnp.where(array[:, :1] == 0, slot_weight, 1.0),
        ))
        chosen.append([
            [jnp.where((chunk == q) & (array == a), pick, 0.0).astype(BF16) for a in range(2)]
            for q in range(z.nch)
        ])
    loads[2].wait()
    loads[3].wait()
    for b in range(z.nblk):
        for w in range(z.window):
            total = jnp.zeros((z.xr, z.cw), F32)
            for q in range(z.nch):
                cols = pl.ds(b * z.block + q * z.cw, z.cw)
                for a, source in ((0, tok), (1, cot)):
                    total += jnp.dot(chosen[w][q][a], source[:, cols], preferred_element_type=F32)
            x[w, b] = (total * scales[w][0]).astype(BF16)

    pl.semaphore_wait(barrier, group - 1 + z.tp - 1)

    sent = []
    for b in range(z.nblk):
        for d in range(1, z.ep):
            to = lax.rem(i + d, z.ep)
            sent.append(pltpu.make_async_remote_copy(
                src_ref=x.at[to // PARTS, b], dst_ref=xin.at[i, b],
                send_sem=x_send.at[d * z.nblk + b], recv_sem=x_recv.at[i * z.nblk + b],
                device_id=(to, e, s), device_id_type=MESH,
            ))
            sent[-1].start()
        for d in range(1, z.tp):
            to = lax.rem(s + d, z.tp)
            cols = pl.ds(pl.multiple_of(to * z.feats + b * z.block, 128), z.block)
            sent.append(pltpu.make_async_remote_copy(
                src_ref=weights.at[:, :, cols],
                dst_ref=wb.at[s, :, :, pl.ds(b * z.block, z.block)],
                send_sem=w_send.at[d * z.nblk + b], recv_sem=w_recv.at[s * z.nblk + b],
                device_id=(i, e, to), device_id_type=MESH,
            ))
            sent[-1].start()

    def right_copy(b, d):
        to = lax.rem(i + d, z.ep)
        return pltpu.make_async_remote_copy(
            src_ref=x.at[to // PARTS, b], dst_ref=rb.at[e, i],
            send_sem=r_send.at[b * z.ep + d], recv_sem=r_recv.at[0],
            device_id=(to, s * z.nblk + b, s), device_id_type=MESH,
        )

    for b in range(z.nblk):
        @pl.when(s * z.nblk + b != e)
        def _():
            for d in range(z.ep):
                right_copy(b, d).start()

    xin[i] = x[i // PARTS]
    for w in range(z.window):
        home = jnp.transpose(picks[w])
        for q in range(z.nch):
            for a in range(2):
                homes[w, 2 * q + a] = jnp.where(
                    (lane_chunk == q) & (lane_array == a), home, 0.0
                ).astype(BF16)
    own_w.wait()
    for copy in loads[4:]:
        copy.wait()

    last = (((1,), (1,)), ((), ()))
    for b in range(z.nblk):
        for d in range(1, z.ep):
            source = lax.rem(i + d, z.ep)
            landed = xin.at[source, b]
            pltpu.make_async_copy(landed, landed, x_recv.at[source * z.nblk + b]).wait()
        flat = jnp.dot(
            perm[...], xin[:, b].reshape(z.ep * z.xr, z.cw), preferred_element_type=F32
        ).astype(BF16)
        block = pl.ds(b * z.block, z.block)
        for q in range(z.nch):
            cols = pl.ds(b * z.block + q * z.cw, z.cw)
            rows[:, cols] = flat[q * 2 * z.rows:(q + 1) * 2 * z.rows]
        for d in range(1, z.tp):
            source = lax.rem(s + d, z.tp)
            landed = wb.at[source, :, :, block]
            pltpu.make_async_copy(landed, landed, w_recv.at[source * z.nblk + b]).wait()
        for m in range(3):
            part = rows[:z.rows, block] if m < 2 else rows[z.rows:, block]
            for t in range(z.tp):
                value = lax.dot_general(part, wb[t, m, :, block], last, preferred_element_type=F32)
                if b:
                    value += pout[m, t]
                pout[m, t] = value
            if b == z.nblk - 1:
                for d in range(1, z.tp):
                    sent.append(pltpu.make_async_remote_copy(
                        src_ref=pout.at[m], dst_ref=pin.at[s, m],
                        send_sem=p_send.at[d * 3 + m], recv_sem=p_recv.at[s * 3 + m],
                        device_id=(i, e, lax.rem(s + d, z.tp)), device_id_type=MESH,
                    ))
                    sent[-1].start()
    for d in range(1, z.tp):
        source = lax.rem(s + d, z.tp)
        for m in range(3):
            landed = pin.at[source, m]
            pltpu.make_async_copy(landed, landed, p_recv.at[source * 3 + m]).wait()

    for t in range(z.tp):
        sums = []
        for m in range(3):
            value = pout[m, t]
            for d in range(1, z.tp):
                value += pin[lax.rem(s + d, z.tp), m, t]
            sums.append(value)
        gate, up, d_hidden = sums
        sig = jax.nn.sigmoid(gate)
        active = gate * sig
        hb[t, 0] = (d_hidden * up * sig * (1.0 + gate * (1.0 - sig))).astype(BF16)
        hb[t, 1] = (d_hidden * active).astype(BF16)
        hb[t, 2] = (active * up).astype(BF16)

    first = (((0,), (0,)), ((), ()))
    packed = jnp.zeros((z.hid, z.lanes), F32)
    for m in range(3):
        packed += lax.dot_general(hb[s, m], place[m], first, preferred_element_type=F32)
    lout[...] = packed.astype(BF16)
    for d in range(1, z.edp):
        sent.append(pltpu.make_async_remote_copy(
            src_ref=lout, dst_ref=lb.at[e], send_sem=l_send.at[d], recv_sem=l_recv.at[e],
            device_id=(i, lax.rem(e + d, z.edp), s), device_id_type=MESH,
        ))
        sent[-1].start()
    left[e] = lout[...]

    for b in range(z.nblk):
        block = pl.ds(b * z.block, z.block)
        out = jnp.zeros((z.rows, z.block), F32)
        back = jnp.zeros((z.rows, z.block), F32)
        for t in range(z.tp):
            out += jnp.dot(hb[t, 2], wb[t, 2, :, block], preferred_element_type=F32)
            back += jnp.dot(hb[t, 0], wb[t, 0, :, block], preferred_element_type=F32)
            back += jnp.dot(hb[t, 1], wb[t, 1, :, block], preferred_element_type=F32)
        ob[:z.rows] = out.astype(BF16)
        ob[z.rows:] = back.astype(BF16)
        total = jnp.zeros((z.ep * z.xr, z.cw), F32)
        for q in range(z.nch):
            total += jnp.dot(perm_t[q], ob[:, q * z.cw:(q + 1) * z.cw], preferred_element_type=F32)
        y[:, b] = total.astype(BF16).reshape(z.ep, z.xr, z.cw)
        for d in range(1, z.ep):
            to = lax.rem(i + d, z.ep)
            sent.append(pltpu.make_async_remote_copy(
                src_ref=y.at[to, b], dst_ref=yin.at[i, b],
                send_sem=y_send.at[d * z.nblk + b], recv_sem=y_recv.at[i * z.nblk + b],
                device_id=(to, e, s), device_id_type=MESH,
            ))
            sent[-1].start()
    yin[i] = y[i]

    owner = e // z.nblk
    mine = e - owner * z.nblk

    def relay(d):
        return pltpu.make_async_remote_copy(
            src_ref=rb, dst_ref=rb, send_sem=q_send.at[d], recv_sem=q_recv.at[0],
            device_id=(i, e, lax.rem(s + d, z.tp)), device_id_type=MESH,
        )

    @pl.when(s == owner)
    def _():
        for source in range(z.ep):
            rb[e, source] = xin[source, mine]
        others = rb.at[pl.ds(0, z.edp - 1)]
        pltpu.make_async_copy(others, others, r_recv.at[0]).wait()
        for d in range(1, z.tp):
            relay(d).start()

    @pl.when(s != owner)
    def _():
        pltpu.make_async_copy(rb, rb, q_recv.at[0]).wait()

    for r in range(z.edp):
        flat = jnp.dot(
            factor[...], rb[r].reshape(z.ep * z.xr, z.cw), preferred_element_type=F32
        ).astype(BF16)
        for q in range(z.nch):
            right[pl.ds(r * z.lanes, z.lanes), pl.ds(q * z.cw, z.cw)] = flat[
                q * z.lanes:(q + 1) * z.lanes
            ]

    for b in range(z.nblk):
        for d in range(1, z.ep):
            source = lax.rem(i + d, z.ep)
            landed = yin.at[source, b]
            pltpu.make_async_copy(landed, landed, y_recv.at[source * z.nblk + b]).wait()
        for w in range(z.window):
            total = yin[w * PARTS, b].astype(F32)
            for h in range(1, PARTS):
                total += yin[w * PARTS + h, b].astype(F32)
            summed[w, b] = (total * scales[w][1]).astype(BF16)

    for d in range(1, z.edp):
        source = lax.rem(e + d, z.edp)
        landed = lb.at[source]
        pltpu.make_async_copy(landed, landed, l_recv.at[source]).wait()
        left[source] = lb[source]

    for copy in sent:
        copy.wait_send()
    for b in range(z.nblk):
        @pl.when(s * z.nblk + b != e)
        def _():
            for d in range(z.ep):
                right_copy(b, d).wait_send()

    @pl.when(s == owner)
    def _():
        for d in range(1, z.tp):
            relay(d).wait_send()


def finish(z, left, right, summed, homes, mixed, grad_tok, wgrad, wg, mix, grad, sem):
    factors = jnp.concatenate([left[r] for r in range(z.edp)], axis=1)
    lane = lax.broadcasted_iota(jnp.int32, (z.hid, z.lanes), 1)
    width = z.ep * CAP
    copies = []
    for m in range(3):
        keep = ((lane >= m * width) & (lane < (m + 1) * width)).astype(F32).astype(BF16)
        keep = jnp.concatenate([keep] * z.edp, axis=1)
        wg[m] = jnp.dot(factors * keep, right[...], preferred_element_type=F32)
        copies.append(pltpu.make_async_copy(wg.at[m], wgrad.at[m], sem.at[m]))
        copies[-1].start()
    for a, target in ((0, mix), (1, grad)):
        for q in range(z.nch):
            for b in range(z.nblk):
                value = jnp.zeros((z.tok_rows, z.cw), F32)
                for w in range(z.window):
                    value += jnp.dot(homes[w, 2 * q + a], summed[w, b], preferred_element_type=F32)
                target[:, b * z.block + q * z.cw:b * z.block + (q + 1) * z.cw] = value.astype(BF16)
        copies.append(pltpu.make_async_copy(target, (mixed, grad_tok)[a], sem.at[3 + a]))
        copies[-1].start()
    for copy in copies:
        copy.wait()


def shards(tokens, cotangent, expert_ids, route_weights, expert_weights):
    z = Sizes(
        lax.axis_size("ep"), lax.axis_size("edp"), lax.axis_size("tp"),
        tokens.shape[0], tokens.shape[1], expert_weights.shape[1],
    )
    tables = [jnp.asarray(table, BF16) for table in permutations(z)]
    operands = [tokens, cotangent, expert_ids.T, route_weights.T] + tables
    vmem = pl.BlockSpec(memory_space=pltpu.VMEM)
    hbm = pl.BlockSpec(memory_space=pltpu.HBM)
    dma = pltpu.SemaphoreType.DMA
    between = (
        jax.ShapeDtypeStruct((z.edp, z.hid, z.lanes), BF16),
        jax.ShapeDtypeStruct((z.edp * z.lanes, z.block), BF16),
        jax.ShapeDtypeStruct((z.window, z.nblk, z.xr, z.cw), BF16),
        jax.ShapeDtypeStruct((z.window, 2 * z.nch, z.tok_rows, z.xr), BF16),
    )
    passed = pl.pallas_call(
        functools.partial(kernel, z),
        out_shape=between,
        in_specs=[hbm] * (len(operands) + 1),
        out_specs=(vmem,) * 4,
        scratch_shapes=[pltpu.VMEM(o.shape, o.dtype) for o in operands] + [
            pltpu.VMEM((z.tp, 3, z.hid, z.feats), BF16),
            pltpu.VMEM((z.window, z.nblk, z.xr, z.cw), BF16),
            pltpu.VMEM((z.ep, z.nblk, z.xr, z.cw), BF16),
            pltpu.VMEM((z.edp, z.ep, z.xr, z.cw), BF16),
            pltpu.VMEM((2 * z.rows, z.feats), BF16),
            pltpu.VMEM((3, z.tp, z.rows, z.hid), F32),
            pltpu.VMEM((z.tp, 3, z.tp, z.rows, z.hid), F32),
            pltpu.VMEM((z.tp, 3, z.rows, z.hid), BF16),
            pltpu.VMEM((z.hid, z.lanes), BF16),
            pltpu.VMEM((z.edp, z.hid, z.lanes), BF16),
            pltpu.VMEM((2 * z.rows, z.block), BF16),
            pltpu.VMEM((z.ep, z.nblk, z.xr, z.cw), BF16),
            pltpu.VMEM((z.ep, z.nblk, z.xr, z.cw), BF16),
            dma((len(operands),)), dma, dma((z.tp * z.nblk,)), dma((z.tp * z.nblk,)),
            dma((z.ep * z.nblk,)), dma((z.ep * z.nblk,)),
            dma((z.nblk * z.ep,)), dma((1,)), dma((z.tp * 3,)), dma((z.tp * 3,)),
            dma((z.edp,)), dma((z.edp,)), dma((z.ep * z.nblk,)), dma((z.ep * z.nblk,)),
            dma((z.tp,)), dma((1,)),
        ],
        compiler_params=pltpu.CompilerParams(
            collective_id=0, has_side_effects=True, vmem_limit_bytes=VMEM_LIMIT
        ),
        name="expert_block",
    )(*operands, expert_weights)
    return pl.pallas_call(
        functools.partial(finish, z),
        out_shape=(
            jax.ShapeDtypeStruct(tokens.shape, BF16),
            jax.ShapeDtypeStruct(tokens.shape, BF16),
            jax.ShapeDtypeStruct((3, z.hid, z.block), F32),
        ),
        in_specs=[vmem] * 4,
        out_specs=(hbm,) * 3,
        scratch_shapes=[
            pltpu.VMEM((3, z.hid, z.block), F32),
            pltpu.VMEM(tokens.shape, BF16),
            pltpu.VMEM(tokens.shape, BF16),
            dma((5,)),
        ],
        compiler_params=pltpu.CompilerParams(vmem_limit_bytes=VMEM_LIMIT),
        name="finish",
    )(*passed)


def solution(mesh):
    placed = (
        P(("ep", "edp"), "tp"),
        P(("ep", "edp"), "tp"),
        P(("ep", "edp"), None),
        P(("ep", "edp"), None),
        P(None, ("ep", "tp"), None),
    )
    return jax.shard_map(
        shards,
        mesh=mesh,
        in_specs=placed,
        out_specs=(P(("ep", "edp"), "tp"), P(("ep", "edp"), "tp"), P(None, ("ep", "tp"), "edp")),
        check_vma=False,
    )
```

```python
import functools

import jax
import jax.numpy as jnp
import numpy as np
from jax import lax
from jax.experimental import pallas as pl
from jax.experimental.pallas import tpu as pltpu
from jax.sharding import PartitionSpec as P

CAP = 10
PARTS = 4
VMEM_LIMIT = 61 * 1024 * 1024
MESH = pl.DeviceIdType.MESH
F32 = jnp.float32
BF16 = jnp.bfloat16


def round_up(value, unit):
    return -(-value // unit) * unit


class Sizes:
    def __init__(self, ep, edp, tp, tok_rows, feats, hid):
        self.ep, self.edp, self.tp = ep, edp, tp
        self.window = ep // PARTS
        self.tok_rows, self.feats, self.hid = tok_rows, feats, hid
        self.block = feats * tp // edp
        self.nblk = feats // self.block
        self.nch = max(1, min(4, self.block // 128))
        self.cw = self.block // self.nch
        self.xr = round_up(2 * CAP * self.nch, 16)
        self.rows = round_up(ep * CAP, 16)
        self.lanes = round_up(3 * ep * CAP, 128)


def permutations(z):
    table = np.zeros((z.nch, 2, z.rows, z.ep, z.xr), np.float32)
    factor = np.zeros((z.nch, z.lanes, z.ep, z.xr), np.float32)
    place = np.zeros((3, z.rows, z.lanes), np.float32)
    for i in range(z.ep):
        for c in range(CAP):
            for q in range(z.nch):
                for a in range(2):
                    table[q, a, i * CAP + c, i, (2 * q + a) * CAP + c] = 1.0
                for m in range(3):
                    factor[q, (m * z.ep + i) * CAP + c, i, (2 * q + m // 2) * CAP + c] = 1.0
            for m in range(3):
                place[m, i * CAP + c, (m * z.ep + i) * CAP + c] = 1.0
    flat = table.reshape(z.nch, 2 * z.rows, z.ep * z.xr)
    return (
        flat.reshape(-1, z.ep * z.xr), np.swapaxes(flat, 1, 2).copy(),
        factor.reshape(-1, z.ep * z.xr), place,
    )


def slot_parts(index, nch):
    chunk = jnp.zeros_like(index)
    for k in range(1, nch):
        chunk += (index >= 2 * CAP * k).astype(jnp.int32)
    rest = index - 2 * CAP * chunk
    array = (rest >= CAP).astype(jnp.int32)
    return chunk, array, rest - CAP * array


def kernel(
    z, tok_in, cot_in, ids_in, rw_in, perm_in, perm_t_in, factor_in, place_in, weights,
    left, right_out, summed_out, homes_out,
    tok, cot, ids, rw, perm, perm_t, factor, place,
    wb, x, xin, rb, rows, pout, pin, hb, lout, lb, ob, y, yin, right, summed, homes,
    out_sem, in_sem, w_loc, w_send, w_recv, x_send, x_recv, r_send, r_recv, p_send, p_recv,
    l_send, l_recv, y_send, y_recv, q_send, q_recv,
):
    i, e, s = lax.axis_index("ep"), lax.axis_index("edp"), lax.axis_index("tp")
    barrier = pltpu.get_barrier_semaphore()
    group = z.ep * z.edp

    loads = [
        pltpu.make_async_copy(source, target, in_sem.at[k])
        for k, (source, target) in enumerate((
            (ids_in, ids), (rw_in, rw), (tok_in, tok), (cot_in, cot),
            (perm_in, perm), (perm_t_in, perm_t), (factor_in, factor), (place_in, place),
        ))
    ]
    for copy in loads[:4]:
        copy.start()

    def greet(step, carry):
        di = step // z.edp
        de = step - di * z.edp
        pl.semaphore_signal(
            barrier, inc=1,
            device_id=(lax.rem(i + di, z.ep), lax.rem(e + de, z.edp), s),
            device_id_type=MESH,
        )
        return carry

    for d in range(1, z.tp):
        pl.semaphore_signal(
            barrier, inc=1, device_id=(i, e, lax.rem(s + d, z.tp)), device_id_type=MESH
        )
    lax.fori_loop(1, group, greet, 0)

    own_w = pltpu.make_async_copy(
        weights.at[:, :, pl.ds(pl.multiple_of(s * z.feats, 128), z.feats)], wb.at[s], w_loc
    )
    own_w.start()
    for copy in loads[4:]:
        copy.start()

    row = lax.broadcasted_iota(jnp.int32, (z.xr, z.tok_rows), 0)
    chunk, array, slot = slot_parts(row, z.nch)
    in_use = row < 2 * CAP * z.nch
    before = (
        lax.broadcasted_iota(jnp.int32, (z.tok_rows, z.tok_rows), 0)
        < lax.broadcasted_iota(jnp.int32, (z.tok_rows, z.tok_rows), 1)
    ).astype(F32).astype(BF16)
    lane = lax.broadcasted_iota(jnp.int32, (z.tok_rows, z.xr), 1)
    lane_chunk, lane_array, _ = slot_parts(lane, z.nch)
    loads[0].wait()
    loads[1].wait()
    ids_t = ids[...]
    rw_t = rw[...]
    chosen, scales, picks = [], [], []
    for w in range(z.window):
        hit = (ids_t == w).astype(F32)
        match = jnp.sum(hit, axis=0, keepdims=True)
        weight = jnp.sum(hit * rw_t, axis=0, keepdims=True)
        match_all = jnp.broadcast_to(match, (z.xr, z.tok_rows))
        rank = jnp.dot(match_all.astype(BF16), before, preferred_element_type=F32)
        pick = jnp.where(in_use & (rank == slot.astype(F32)), match_all, 0.0)
        slot_weight = jnp.sum(pick * weight, axis=1, keepdims=True)
        picks.append(pick)
        scales.append((
            jnp.where(array[:, :1] == 1, slot_weight, 1.0), jnp.where(array[:, :1] == 0, slot_weight, 1.0),
        ))
        chosen.append([
            [jnp.where((chunk == q) & (array == a), pick, 0.0).astype(BF16) for a in range(2)]
            for q in range(z.nch)
        ])
    pl.semaphore_wait(barrier, group - 1 + z.tp - 1)

    sent = []
    for b in range(z.nblk):
        for d in range(1, z.tp):
            to = lax.rem(s + d, z.tp)
            cols = pl.ds(pl.multiple_of(to * z.feats + b * z.block, 128), z.block)
            sent.append(pltpu.make_async_remote_copy(
                src_ref=weights.at[:, :, cols],
                dst_ref=wb.at[s, :, :, pl.ds(b * z.block, z.block)],
                send_sem=w_send.at[d * z.nblk + b], recv_sem=w_recv.at[s * z.nblk + b],
                device_id=(i, e, to), device_id_type=MESH,
            ))
            sent[-1].start()
    loads[2].wait()
    loads[3].wait()
    for b in range(z.nblk):
        for w in range(z.window):
            total = jnp.zeros((z.xr, z.cw), F32)
            for q in range(z.nch):
                cols = pl.ds(b * z.block + q * z.cw, z.cw)
                for a, source in ((0, tok), (1, cot)):
                    total += jnp.dot(chosen[w][q][a], source[:, cols], preferred_element_type=F32)
            x[w, b] = (total * scales[w][0]).astype(BF16)
        for d in range(1, z.ep):
            to = lax.rem(i + d, z.ep)
            sent.append(pltpu.make_async_remote_copy(
                src_ref=x.at[to // PARTS, b], dst_ref=xin.at[i, b],
                send_sem=x_send.at[d * z.nblk + b], recv_sem=x_recv.at[i * z.nblk + b],
                device_id=(to, e, s), device_id_type=MESH,
            ))
            sent[-1].start()

    def right_copy(b, d):
        to = lax.rem(i + d, z.ep)
        return pltpu.make_async_remote_copy(
            src_ref=x.at[to // PARTS, b], dst_ref=rb.at[e, i],
            send_sem=r_send.at[b * z.ep + d], recv_sem=r_recv.at[0],
            device_id=(to, s * z.nblk + b, s), device_id_type=MESH,
        )

    for b in range(z.nblk):
        @pl.when(s * z.nblk + b != e)
        def _():
            for d in range(z.ep):
                right_copy(b, d).start()

    xin[i] = x[i // PARTS]
    for w in range(z.window):
        home = jnp.transpose(picks[w])
        for q in range(z.nch):
            for a in range(2):
                homes[w, 2 * q + a] = jnp.where(
                    (lane_chunk == q) & (lane_array == a), home, 0.0
                ).astype(BF16)
    own_w.wait()
    for copy in loads[4:]:
        copy.wait()

    last = (((1,), (1,)), ((), ()))
    for b in range(z.nblk):
        for d in range(1, z.ep):
            source = lax.rem(i + d, z.ep)
            landed = xin.at[source, b]
            pltpu.make_async_copy(landed, landed, x_recv.at[source * z.nblk + b]).wait()
        flat = jnp.dot(
            perm[...], xin[:, b].reshape(z.ep * z.xr, z.cw), preferred_element_type=F32
        ).astype(BF16)
        block = pl.ds(b * z.block, z.block)
        for q in range(z.nch):
            cols = pl.ds(b * z.block + q * z.cw, z.cw)
            rows[:, cols] = flat[q * 2 * z.rows:(q + 1) * 2 * z.rows]
        for d in range(1, z.tp):
            source = lax.rem(s + d, z.tp)
            landed = wb.at[source, :, :, block]
            pltpu.make_async_copy(landed, landed, w_recv.at[source * z.nblk + b]).wait()
        for m in range(3):
            part = rows[:z.rows, block] if m < 2 else rows[z.rows:, block]
            for t in range(z.tp):
                value = lax.dot_general(part, wb[t, m, :, block], last, preferred_element_type=F32)
                if b:
                    value += pout[m, t]
                pout[m, t] = value
            if b == z.nblk - 1:
                for d in range(1, z.tp):
                    sent.append(pltpu.make_async_remote_copy(
                        src_ref=pout.at[m], dst_ref=pin.at[s, m],
                        send_sem=p_send.at[d * 3 + m], recv_sem=p_recv.at[s * 3 + m],
                        device_id=(i, e, lax.rem(s + d, z.tp)), device_id_type=MESH,
                    ))
                    sent[-1].start()
    for d in range(1, z.tp):
        source = lax.rem(s + d, z.tp)
        for m in range(3):
            landed = pin.at[source, m]
            pltpu.make_async_copy(landed, landed, p_recv.at[source * 3 + m]).wait()

    for t in range(z.tp):
        sums = []
        for m in range(3):
            value = pout[m, t]
            for d in range(1, z.tp):
                value += pin[lax.rem(s + d, z.tp), m, t]
            sums.append(value)
        gate, up, d_hidden = sums
        sig = jax.nn.sigmoid(gate)
        active = gate * sig
        hb[t, 0] = (d_hidden * up * sig * (1.0 + gate * (1.0 - sig))).astype(BF16)
        hb[t, 1] = (d_hidden * active).astype(BF16)
        hb[t, 2] = (active * up).astype(BF16)

    first = (((0,), (0,)), ((), ()))
    packed = jnp.zeros((z.hid, z.lanes), F32)
    for m in range(3):
        packed += lax.dot_general(hb[s, m], place[m], first, preferred_element_type=F32)
    lout[...] = packed.astype(BF16)
    for d in range(1, z.edp):
        sent.append(pltpu.make_async_remote_copy(
            src_ref=lout, dst_ref=lb.at[e], send_sem=l_send.at[d], recv_sem=l_recv.at[e],
            device_id=(i, lax.rem(e + d, z.edp), s), device_id_type=MESH,
        ))
        sent[-1].start()
    written = [pltpu.make_async_copy(lout, left.at[e], out_sem.at[0])]
    written[-1].start()

    owner = e // z.nblk
    mine = e - owner * z.nblk

    def relay(d):
        return pltpu.make_async_remote_copy(
            src_ref=rb, dst_ref=rb, send_sem=q_send.at[d], recv_sem=q_recv.at[0],
            device_id=(i, e, lax.rem(s + d, z.tp)), device_id_type=MESH,
        )

    @pl.when(s == owner)
    def _():
        for source in range(z.ep):
            rb[e, source] = xin[source, mine]
        others = rb.at[pl.ds(0, z.edp - 1)]
        pltpu.make_async_copy(others, others, r_recv.at[0]).wait()
        for d in range(1, z.tp):
            relay(d).start()

    for b in range(z.nblk):
        block = pl.ds(b * z.block, z.block)
        out = jnp.zeros((z.rows, z.block), F32)
        back = jnp.zeros((z.rows, z.block), F32)
        for t in range(z.tp):
            out += jnp.dot(hb[t, 2], wb[t, 2, :, block], preferred_element_type=F32)
            back += jnp.dot(hb[t, 0], wb[t, 0, :, block], preferred_element_type=F32)
            back += jnp.dot(hb[t, 1], wb[t, 1, :, block], preferred_element_type=F32)
        ob[:z.rows] = out.astype(BF16)
        ob[z.rows:] = back.astype(BF16)
        total = jnp.zeros((z.ep * z.xr, z.cw), F32)
        for q in range(z.nch):
            total += jnp.dot(perm_t[q], ob[:, q * z.cw:(q + 1) * z.cw], preferred_element_type=F32)
        y[:, b] = total.astype(BF16).reshape(z.ep, z.xr, z.cw)
        for d in range(1, z.ep):
            to = lax.rem(i + d, z.ep)
            sent.append(pltpu.make_async_remote_copy(
                src_ref=y.at[to, b], dst_ref=yin.at[i, b],
                send_sem=y_send.at[d * z.nblk + b], recv_sem=y_recv.at[i * z.nblk + b],
                device_id=(to, e, s), device_id_type=MESH,
            ))
            sent[-1].start()
    yin[i] = y[i]

    @pl.when(s != owner)
    def _():
        pltpu.make_async_copy(rb, rb, q_recv.at[0]).wait()

    for r in range(z.edp):
        flat = jnp.dot(
            factor[...], rb[r].reshape(z.ep * z.xr, z.cw), preferred_element_type=F32
        ).astype(BF16)
        for q in range(z.nch):
            right[pl.ds(r * z.lanes, z.lanes), pl.ds(q * z.cw, z.cw)] = flat[
                q * z.lanes:(q + 1) * z.lanes
            ]
    for k, (source, target) in enumerate(((homes, homes_out), (right, right_out))):
        written.append(pltpu.make_async_copy(source, target, out_sem.at[z.edp + k]))
        written[-1].start()

    for b in range(z.nblk):
        for d in range(1, z.ep):
            source = lax.rem(i + d, z.ep)
            landed = yin.at[source, b]
            pltpu.make_async_copy(landed, landed, y_recv.at[source * z.nblk + b]).wait()
        for w in range(z.window):
            total = yin[w * PARTS, b].astype(F32)
            for h in range(1, PARTS):
                total += yin[w * PARTS + h, b].astype(F32)
            summed[w, b] = (total * scales[w][1]).astype(BF16)
    written.append(pltpu.make_async_copy(summed, summed_out, out_sem.at[z.edp + 2]))
    written[-1].start()

    for d in range(1, z.edp):
        source = lax.rem(e + d, z.edp)
        landed = lb.at[source]
        pltpu.make_async_copy(landed, landed, l_recv.at[source]).wait()
        written.append(pltpu.make_async_copy(landed, left.at[source], out_sem.at[d]))
        written[-1].start()

    for copy in sent:
        copy.wait_send()
    for copy in written:
        copy.wait()
    for b in range(z.nblk):
        @pl.when(s * z.nblk + b != e)
        def _():
            for d in range(z.ep):
                right_copy(b, d).wait_send()

    @pl.when(s == owner)
    def _():
        for d in range(1, z.tp):
            relay(d).wait_send()


def finish(
    z, left_in, right_in, summed_in, homes_in, mixed, grad_tok, wgrad,
    left, right, summed, homes, wg, mix, grad, in_sem, sem,
):
    loads = [
        pltpu.make_async_copy(source, target, in_sem.at[k])
        for k, (source, target) in enumerate(
            ((summed_in, summed), (homes_in, homes), (left_in, left), (right_in, right))
        )
    ]
    for copy in loads:
        copy.start()
    lane = lax.broadcasted_iota(jnp.int32, (1, z.lanes), 1)
    width = z.ep * CAP
    keeps = [((lane >= m * width) & (lane < (m + 1) * width)).astype(F32).astype(BF16) for m in range(3)]
    loads[0].wait()
    loads[1].wait()
    copies = []
    for b in range(z.nblk):
        value = jnp.zeros((2 * z.nch * z.tok_rows, z.cw), F32)
        for w in range(z.window):
            home = homes[w].reshape(2 * z.nch * z.tok_rows, z.xr)
            value += jnp.dot(home, summed[w, b], preferred_element_type=F32)
        for q in range(z.nch):
            cols = pl.ds(b * z.block + q * z.cw, z.cw)
            for a, target in ((0, mix), (1, grad)):
                at = (2 * q + a) * z.tok_rows
                target[:, cols] = value[at:at + z.tok_rows].astype(BF16)
    for a, target in ((0, mix), (1, grad)):
        copies.append(pltpu.make_async_copy(target, (mixed, grad_tok)[a], sem.at[3 + a]))
        copies[-1].start()
    loads[2].wait()
    loads[3].wait()
    for m in range(3):
        factors = jnp.concatenate([left[r] * keeps[m] for r in range(z.edp)], axis=1)
        wg[m] = jnp.dot(factors, right[...], preferred_element_type=F32)
        copies.append(pltpu.make_async_copy(wg.at[m], wgrad.at[m], sem.at[m]))
        copies[-1].start()
    for copy in copies:
        copy.wait()


def shards(tokens, cotangent, expert_ids, route_weights, expert_weights):
    z = Sizes(
        lax.axis_size("ep"), lax.axis_size("edp"), lax.axis_size("tp"),
        tokens.shape[0], tokens.shape[1], expert_weights.shape[1],
    )
    tables = [jnp.asarray(table, BF16) for table in permutations(z)]
    operands = [tokens, cotangent, expert_ids.T, route_weights.T] + tables
    hbm = pl.BlockSpec(memory_space=pltpu.HBM)
    dma = pltpu.SemaphoreType.DMA
    between = (
        jax.ShapeDtypeStruct((z.edp, z.hid, z.lanes), BF16),
        jax.ShapeDtypeStruct((z.edp * z.lanes, z.block), BF16),
        jax.ShapeDtypeStruct((z.window, z.nblk, z.xr, z.cw), BF16),
        jax.ShapeDtypeStruct((z.window, 2 * z.nch, z.tok_rows, z.xr), BF16),
    )
    passed = pl.pallas_call(
        functools.partial(kernel, z),
        out_shape=between,
        in_specs=[hbm] * (len(operands) + 1),
        out_specs=(hbm,) * 4,
        scratch_shapes=[pltpu.VMEM(o.shape, o.dtype) for o in operands] + [
            pltpu.VMEM((z.tp, 3, z.hid, z.feats), BF16),
            pltpu.VMEM((z.window, z.nblk, z.xr, z.cw), BF16),
            pltpu.VMEM((z.ep, z.nblk, z.xr, z.cw), BF16),
            pltpu.VMEM((z.edp, z.ep, z.xr, z.cw), BF16),
            pltpu.VMEM((2 * z.rows, z.feats), BF16),
            pltpu.VMEM((3, z.tp, z.rows, z.hid), F32),
            pltpu.VMEM((z.tp, 3, z.tp, z.rows, z.hid), F32),
            pltpu.VMEM((z.tp, 3, z.rows, z.hid), BF16),
            pltpu.VMEM((z.hid, z.lanes), BF16),
            pltpu.VMEM((z.edp, z.hid, z.lanes), BF16),
            pltpu.VMEM((2 * z.rows, z.block), BF16),
            pltpu.VMEM((z.ep, z.nblk, z.xr, z.cw), BF16),
            pltpu.VMEM((z.ep, z.nblk, z.xr, z.cw), BF16),
        ] + [pltpu.VMEM(o.shape, o.dtype) for o in between[1:]] + [
            dma((z.edp + 3,)), dma((len(operands),)), dma, dma((z.tp * z.nblk,)), dma((z.tp * z.nblk,)),
            dma((z.ep * z.nblk,)), dma((z.ep * z.nblk,)),
            dma((z.nblk * z.ep,)), dma((1,)), dma((z.tp * 3,)), dma((z.tp * 3,)),
            dma((z.edp,)), dma((z.edp,)), dma((z.ep * z.nblk,)), dma((z.ep * z.nblk,)),
            dma((z.tp,)), dma((1,)),
        ],
        compiler_params=pltpu.CompilerParams(
            collective_id=0, has_side_effects=True, vmem_limit_bytes=VMEM_LIMIT
        ),
        name="expert_block",
    )(*operands, expert_weights)
    return pl.pallas_call(
        functools.partial(finish, z),
        out_shape=(
            jax.ShapeDtypeStruct(tokens.shape, BF16),
            jax.ShapeDtypeStruct(tokens.shape, BF16),
            jax.ShapeDtypeStruct((3, z.hid, z.block), F32),
        ),
        in_specs=[hbm] * 4,
        out_specs=(hbm,) * 3,
        scratch_shapes=[pltpu.VMEM(o.shape, o.dtype) for o in between] + [
            pltpu.VMEM((3, z.hid, z.block), F32),
            pltpu.VMEM(tokens.shape, BF16),
            pltpu.VMEM(tokens.shape, BF16),
            dma((4,)), dma((5,)),
        ],
        compiler_params=pltpu.CompilerParams(vmem_limit_bytes=VMEM_LIMIT),
        name="finish",
    )(*passed)


def solution(mesh):
    placed = (
        P(("ep", "edp"), "tp"),
        P(("ep", "edp"), "tp"),
        P(("ep", "edp"), None),
        P(("ep", "edp"), None),
        P(None, ("ep", "tp"), None),
    )
    return jax.shard_map(
        shards,
        mesh=mesh,
        in_specs=placed,
        out_specs=(P(("ep", "edp"), "tp"), P(("ep", "edp"), "tp"), P(None, ("ep", "tp"), "edp")),
        check_vma=False,
    )
```
